32 devices in a mesh: section: 2 (over core), dp: 16 (over z, y, x).
Axes of the slice: x: 2, y: 2, z: 4, core: 2. Of those that a mesh axis runs over, the one named last changes fastest.
Arguments:
- activations: bfloat16 [32, 6, 192, 2560], P(('section', 'dp')), parts along dimension 0, may hold values from -6 to 6
- cotangents: bfloat16 [32, 6, 192, 2560], P(('section', 'dp')), parts along dimension 0, may hold values from -1.5 to 1.5
- failed: int32 [1], replicated, may hold values from 0 to 15
- counts: int32 [16], P('dp'), may hold values from 1 to 6, as said below
- order: int32 [16, 6], P('dp'), may hold values from 0 to 5, each once within a row
Outputs:
- gradient: float32 [5120, 2560], P(('section', 'dp')), parts along dimension 0
The draws below stay inside these ranges and needn't reach their ends.
There are 2 independent parts, one for each index of `section`. The reference program is written for one: setup_inputs(seed, part) draws one part's arguments, and reference() takes and returns one part's arrays. A program takes and returns all parts, laid end to end along the dimension named above; an argument that names none is the same for every part. Nothing has to cross between parts.
Inputs may be any that keep to these rules, and one draw needn't show every extreme that they name: `counts`: each replica reports 1 to 6 micro-batches; some replica reports exactly 6.
All inputs are finite; a program needn't handle non-finite values.
Results may differ from the reference program's by a relative error of at most 0.0003.
Values sent between devices are 32-bit elements; how exact they have to be, the bound alone decides.
A program may use at most 320 MiB of HBM per device.

```python
import jax
import jax.numpy as jnp

IN = 2560
OUT = 2560
M = 192
SLOTS = 6
DP = 16


def draw_counts(key, part):
    reported = jax.random.randint(jax.random.fold_in(key, 11), (DP,), 1, SLOTS + 1)
    busiest = jax.random.randint(jax.random.fold_in(key, 12), (), 0, DP)
    replica_group = jnp.arange(DP, dtype=jnp.int32)
    return jnp.where(replica_group == busiest, SLOTS, reported).astype(jnp.int32)


def strengthened(entries, key, source, target, parts, factor):
    owner, partner = [(jnp.arange(entries.shape[axis_at]) // (entries.shape[axis_at] // parts)).reshape([-1 if axis == axis_at else 1 for axis in range(entries.ndim)]) for axis_at in (source, target)]
    chosen = jax.random.permutation(key, parts)[partner]
    strong = (owner == chosen) | (owner == (partner + parts // 2) % parts)
    return jnp.where(strong, factor * entries, entries)


def steps_of(own_key, shape, pieces, smallest, high):
    def one(dim, shards_of):
        steps = jax.random.uniform(jax.random.fold_in(jax.random.fold_in(own_key, 6), dim), (shards_of,), jnp.float32, smallest / len(pieces), high / len(pieces))
        return jnp.repeat(jnp.exp(steps), shape[dim] // shards_of).reshape((-1,) + (1,) * (len(shape) - dim - 1))

    loudness = one(*pieces[0])
    for cut in pieces[1:]:
        loudness = loudness * one(*cut)
    return loudness


def noise(own_key, dims, deviation, most, cuts=(), held_as=jnp.bfloat16):
    array = jax.random.normal(own_key, dims, jnp.float32) * deviation
    if len(cuts) > 0:
        array = steps_of(own_key, dims, cuts, -0.22, 0.18) * array
    return jnp.clip(array, min=-most, max=most).astype(held_as)


def gaussian_with(rng, shape, width, bound, shards, heavy, held_as=jnp.bfloat16):
    array = width * jax.random.normal(rng, shape, jnp.float32)
    if shards:
        array = array * steps_of(rng, shape, shards, -0.22, 0.18)
    return jnp.clip(strengthened(array, jax.random.fold_in(rng, 3), *heavy), -bound, bound).astype(held_as)


def setup_inputs(seed: int = 0, part: int = 0) -> dict:
    seeds = jax.random.split(jax.random.key(seed), 6)
    part_keys = jax.random.split(jax.random.fold_in(seeds[5], part), 6)
    return {
        "activations": gaussian_with(part_keys[0], (DP, SLOTS, M, IN), 1.0, 6.0, ((0, 16),), (0, 3, 16, 2.0)),
        "cotangents": noise(part_keys[1], (DP, SLOTS, M, OUT), 0.25, 1.5, ((0, 16),)),
        "failed": jax.random.randint(seeds[2], (1,), 0, DP).astype(jnp.int32),
        "counts": draw_counts(jax.random.fold_in(seeds[5], 71), part),
        "order": jax.vmap(lambda own: jax.random.permutation(own, SLOTS))(jax.random.split(seeds[4], DP)).reshape((DP, SLOTS)).astype(jnp.int32),
    }


def reference(activations, cotangents, failed, counts, order):
    partial_gradient = jnp.zeros((IN, OUT), jnp.float32)
    for replica in range(DP):
        for position in range(SLOTS):
            selected_replica = order[replica, position]
            live = jnp.logical_and(position < counts[replica], replica != failed[0])
            weight_live = jnp.where(live, 1.0, 0.0).astype(jnp.bfloat16)
            act_rows = activations[replica, selected_replica]
            cot_rows = cotangents[replica, selected_replica] * weight_live
            partial_gradient = partial_gradient + jnp.dot(act_rows.T, cot_rows, preferred_element_type=jnp.float32)
    replica_group = jnp.arange(DP, dtype=jnp.int32)
    remaining_replica_total = jnp.sum(jnp.where(replica_group != failed[0], counts, 0)).astype(jnp.float32)
    return partial_gradient / remaining_replica_total
```

```python
import jax
import jax.numpy as jnp
from jax import lax
from jax.sharding import PartitionSpec as P


CHUNKS = 4


def solution(mesh):
    replicas = mesh.shape["dp"]
    bits = replicas.bit_length() - 1
    assert replicas == 1 << bits
    third = max(bits // 3, 1)
    x_bits = list(range(0, third))
    y_bits = list(range(third, third + (bits - third) // 2))
    z_bits = list(range(third + (bits - third) // 2, bits))
    orders = (
        x_bits[::-1] + y_bits[::-1] + z_bits[::-1],
        y_bits[::-1] + x_bits[::-1] + z_bits[::-1],
    )

    def swap(value, bit):
        return lax.ppermute(value, "dp", [(i, i ^ (1 << bit)) for i in range(replicas)])

    def shards(activations, cotangents, failed, counts, order):
        me = lax.axis_index("dp")
        alive = jnp.where(me == failed[0], 0, counts[0])
        total = alive.astype(jnp.float32).reshape(1)
        for bit in range(bits):
            total = total + swap(total, bit)
        _, slots, tokens, width = activations.shape
        out_width = cotangents.shape[3]
        rows = width // replicas
        positions = jnp.arange(slots, dtype=jnp.int32)
        live = jnp.sum(
            jnp.where(
                (order[0][None, :] == positions[:, None]) & (positions < alive)[None, :], 1.0, 0.0
            ),
            axis=1,
        ).astype(jnp.bfloat16)
        act = activations[0].reshape(slots * tokens, width)
        cot = (cotangents[0] * live[:, None, None]).reshape(slots * tokens, out_width)
        act_t = act.T.reshape((2,) * bits + (rows, slots * tokens))

        def pick(value, left, bit, index):
            return lax.dynamic_index_in_dim(value, index, left.index(bit), keepdims=False)

        def mine(bit):
            return (me >> bit) & 1

        def product(lhs, rhs):
            return lax.dot_general(
                lhs, rhs, (((lhs.ndim - 1,), (0,)), ((), ())), preferred_element_type=jnp.float32
            )

        piece = out_width // (len(orders) * CHUNKS)
        columns = {}
        state = {}
        names = [(c, o) for c in range(CHUNKS) for o in range(len(orders))]
        halves = []
        for route in orders:
            left = list(range(bits))[::-1]
            first = route[0]
            halves.append(
                (pick(act_t, left, first, 1 - mine(first)), pick(act_t, left, first, mine(first)))
            )
        for c, o in names:
            start = (o * CHUNKS + c) * piece
            part = cot[:, start : start + piece]
            send, keep = halves[o]
            got = swap(product(send, part), orders[o][0])
            held = product(keep, part) + got
            left = [b for b in range(bits)[::-1] if b != orders[o][0]]
            state[c, o] = (held, left)
        for step in range(1, bits):
            for c, o in names:
                held, left = state[c, o]
                bit = orders[o][step]
                got = swap(pick(held, left, bit, 1 - mine(bit)), bit)
                held = pick(held, left, bit, mine(bit)) + got
                state[c, o] = (held, [b for b in left if b != bit])
        for c, o in names:
            columns[o * CHUNKS + c] = state[c, o][0] / total
        return jnp.concatenate([columns[i] for i in range(len(names))], axis=1)

    in_specs = (
        P(("section", "dp"), None, None, None),
        P(("section", "dp"), None, None, None),
        P(),
        P("dp"),
        P("dp", None),
    )
    out_specs = P(("section", "dp"), None)
    return jax.shard_map(shards, mesh=mesh, in_specs=in_specs, out_specs=out_specs, check_vma=False)
```

```python
import jax
import jax.numpy as jnp
from jax import lax
from jax.sharding import PartitionSpec as P


CHUNKS = 4
LANES = 128


def solution(mesh):
    replicas = mesh.shape["dp"]
    bits = replicas.bit_length() - 1
    assert replicas == 1 << bits
    third = max(bits // 3, 1)
    x_bits = list(range(0, third))
    y_bits = list(range(third, third + (bits - third) // 2))
    z_bits = list(range(third + (bits - third) // 2, bits))
    orders = (
        x_bits[::-1] + y_bits[::-1] + z_bits[::-1],
        y_bits[::-1] + x_bits[::-1] + z_bits[::-1],
        z_bits[::-1] + x_bits[::-1] + y_bits[::-1],
    )

    def swap(value, bit):
        return lax.ppermute(value, "dp", [(i, i ^ (1 << bit)) for i in range(replicas)])

    def shards(activations, cotangents, failed, counts, order):
        me = lax.axis_index("dp")
        alive = jnp.where(me == failed[0], 0, counts[0])
        total = alive.astype(jnp.float32).reshape(1)
        for bit in range(bits):
            total = total + swap(total, bit)
        _, slots, tokens, width = activations.shape
        out_width = cotangents.shape[3]
        rows = width // replicas
        positions = jnp.arange(slots, dtype=jnp.int32)
        live = jnp.sum(
            jnp.where(
                (order[0][None, :] == positions[:, None]) & (positions < alive)[None, :], 1.0, 0.0
            ),
            axis=1,
        ).astype(jnp.bfloat16)
        act = activations[0].reshape(slots * tokens, width)
        cot = (cotangents[0] * live[:, None, None]).reshape(slots * tokens, out_width)
        act_t = act.T.reshape((2,) * bits + (rows, slots * tokens))
        cot, total = lax.optimization_barrier((cot, total))

        def pick(value, left, bit, index):
            return lax.dynamic_index_in_dim(value, index, left.index(bit), keepdims=False)

        def mine(bit):
            return (me >> bit) & 1

        def product(lhs, rhs):
            return lax.dot_general(
                lhs, rhs, (((lhs.ndim - 1,), (0,)), ((), ())), preferred_element_type=jnp.float32
            )

        tiles = out_width // LANES
        last = tiles // 10
        side = (tiles - last) // 2
        last = tiles - 2 * side
        pieces = []
        start = 0
        for route, size, cuts in ((2, last, 1), (0, side, CHUNKS), (1, side, CHUNKS)):
            for c in range(cuts):
                wide = size // cuts + (size % cuts if c == 0 else 0)
                pieces.append((c, route, start, wide * LANES))
                start += wide * LANES
        issue = sorted(pieces, key=lambda p: (p[0], p[1] != 2, p[1]))
        everything = list(range(bits))[::-1]
        sent = {}
        state = {}

        def advance(held, left, c, r, step):
            bit = orders[r][step]
            out = pick(held, left, bit, 1 - mine(bit))
            if step == 1:
                sent[c, r] = out
            got = swap(out, bit)
            return pick(held, left, bit, mine(bit)) + got, [b for b in left if b != bit]

        for c, r, start, wide in issue:
            part = lax.slice_in_dim(cot, start, start + wide, axis=1)
            before = (c - 2, 1 - r)
            if before in sent:
                part, sent[before] = lax.optimization_barrier((part, sent[before]))
            bit = orders[r][0]
            send = pick(act_t, everything, bit, 1 - mine(bit))
            keep = pick(act_t, everything, bit, mine(bit))
            got = swap(product(send, part), bit)
            held, left = product(keep, part) + got, [b for b in everything if b != bit]
            held, left = advance(held, left, c, r, 1)
            for step in range(2, bits):
                held, left = advance(held, left, c, r, step)
            state[start] = held / total
        return jnp.concatenate([state[p[2]] for p in pieces], axis=1)

    in_specs = (
        P(("section", "dp"), None, None, None),
        P(("section", "dp"), None, None, None),
        P(),
        P("dp"),
        P("dp", None),
    )
    out_specs = P(("section", "dp"), None)
    return jax.shard_map(shards, mesh=mesh, in_specs=in_specs, out_specs=out_specs, check_vma=False)
```
